32 devices in a mesh: dp: 1 (over z), tp: 4 (over y), sp: 8 (over x, core).
Axes of the slice: x: 4, y: 4, z: 1, core: 2. Of those that a mesh axis runs over, the one named last changes fastest.
The devices are a block of a 4x4x8 slice.
Arguments:
- hidden: bfloat16 [256, 4096], P('dp')
- ln_gain: bfloat16 [4096], replicated
- ln_bias: bfloat16 [4096], replicated
- w_q: bfloat16 [4096, 4096], P(None, 'tp')
- w_k: bfloat16 [4096, 1024], P(None, 'tp')
- w_v: bfloat16 [4096, 1024], P(None, 'tp')
- w_o: bfloat16 [4096, 4096], P('tp')
- k_cache: bfloat16 [256, 1024, 8, 128], P('dp', 'sp', 'tp')
- v_cache: bfloat16 [256, 1024, 8, 128], P('dp', 'sp', 'tp')
- lengths: int32 [256], P('dp')
Outputs:
- output 1: bfloat16 [256, 4096], P('dp')
- output 2: bfloat16 [256, 8, 128], P('dp', 'tp')
- output 3: bfloat16 [256, 8, 128], P('dp', 'tp')
All inputs are finite; a program needn't handle non-finite values.
Results may differ from the reference program's by a relative error of at most 0.0043512.
Values sent between devices are 32-bit elements.
A program may use at most 768 MiB of HBM per device.

```python
import jax
import jax.numpy as jnp
from jax import lax

D_MODEL = 4096
Q_HEADS = 32
KV_HEADS = 8
HEAD_DIM = 128
BATCH_ROWS = 256
SEQ_LEN = 1024
GROUP_SIZE = Q_HEADS // KV_HEADS
ROT_DIM = HEAD_DIM // 2


def norm_one_plus(hidden, ln_gain, ln_bias):
    wide = hidden.astype(jnp.float32)
    row_mean = jnp.mean(wide, axis=-1, keepdims=True)
    centred = wide - row_mean
    row_var = jnp.mean(centred * centred, axis=-1, keepdims=True)
    scaled = centred * lax.rsqrt(row_var + 1e-5)
    return (scaled * (1.0 + ln_gain.astype(jnp.float32)) + ln_bias.astype(jnp.float32)).astype(jnp.bfloat16)


def rotate_first(head_vecs, rot_pos):
    half_rot = ROT_DIM // 2
    inv_freq = 10000.0 ** (-2.0 * jnp.arange(half_rot, dtype=jnp.float32) / ROT_DIM)
    rot_angle = rot_pos.astype(jnp.float32)[..., None] * inv_freq
    cos_part = jnp.cos(rot_angle)
    sin_part = jnp.sin(rot_angle)
    lead_part = head_vecs[..., :half_rot]
    tail_part = head_vecs[..., half_rot:ROT_DIM]
    return jnp.concatenate([lead_part * cos_part - tail_part * sin_part, tail_part * cos_part + lead_part * sin_part, head_vecs[..., ROT_DIM:]], axis=-1)


def setup_inputs(seed: int = 0, part: int = 0) -> dict:
    shared_keys = jax.random.split(jax.random.key(seed), 6)
    part_keys = jax.random.split(jax.random.fold_in(jax.random.key(seed), part), 6)
    q_width = Q_HEADS * HEAD_DIM
    kv_width = KV_HEADS * HEAD_DIM
    seg_count = 16
    seg_len = SEQ_LEN // seg_count
    hidden = jax.random.normal(part_keys[0], (BATCH_ROWS, D_MODEL), jnp.float32)
    ln_gain = 0.5 * jax.random.normal(shared_keys[0], (D_MODEL,), jnp.float32)
    ln_bias = 0.5 * jax.random.normal(shared_keys[1], (D_MODEL,), jnp.float32)
    w_q = jax.random.normal(shared_keys[2], (D_MODEL, q_width), jnp.float32) * D_MODEL ** -0.5
    w_k = jax.random.normal(shared_keys[3], (D_MODEL, kv_width), jnp.float32) * D_MODEL ** -0.5
    w_v = jax.random.normal(shared_keys[4], (D_MODEL, kv_width), jnp.float32) * D_MODEL ** -0.5
    w_o = jax.random.normal(shared_keys[5], (q_width, D_MODEL), jnp.float32) * q_width ** -0.5
    seg_shape = (BATCH_ROWS, seg_count, 1, KV_HEADS, HEAD_DIM)
    full_shape = (BATCH_ROWS, seg_count, seg_len, KV_HEADS, HEAD_DIM)
    cache_shape = (BATCH_ROWS, SEQ_LEN, KV_HEADS, HEAD_DIM)
    k_cache = (jax.random.normal(part_keys[1], seg_shape, jnp.float32) + jax.random.normal(part_keys[2], full_shape, jnp.float32)).reshape(cache_shape)
    v_cache = (1.5 * jax.random.normal(part_keys[3], seg_shape, jnp.float32) + 0.5 * jax.random.normal(part_keys[4], full_shape, jnp.float32)).reshape(cache_shape)
    lengths = jax.random.randint(part_keys[5], (BATCH_ROWS,), SEQ_LEN // 8, SEQ_LEN, dtype=jnp.int32)
    lengths = lengths.at[0].set(SEQ_LEN - 1).at[BATCH_ROWS - 1].set(SEQ_LEN // 8)
    return {'hidden': hidden.astype(jnp.bfloat16), 'ln_gain': ln_gain.astype(jnp.bfloat16), 'ln_bias': ln_bias.astype(jnp.bfloat16), 'w_q': w_q.astype(jnp.bfloat16), 'w_k': w_k.astype(jnp.bfloat16), 'w_v': w_v.astype(jnp.bfloat16), 'w_o': w_o.astype(jnp.bfloat16), 'k_cache': k_cache.astype(jnp.bfloat16), 'v_cache': v_cache.astype(jnp.bfloat16), 'lengths': lengths}


def reference(hidden, ln_gain, ln_bias, w_q, w_k, w_v, w_o, k_cache, v_cache, lengths):
    normed = norm_one_plus(hidden, ln_gain, ln_bias)
    q_proj = jnp.dot(normed, w_q, preferred_element_type=jnp.float32).reshape(BATCH_ROWS, KV_HEADS, GROUP_SIZE, HEAD_DIM)
    queries = rotate_first(q_proj, lengths[:, None, None]).astype(jnp.bfloat16)
    k_proj = jnp.dot(normed, w_k, preferred_element_type=jnp.float32).reshape(BATCH_ROWS, KV_HEADS, HEAD_DIM)
    k_new = rotate_first(k_proj, lengths[:, None]).astype(jnp.bfloat16)
    v_new = jnp.dot(normed, w_v, preferred_element_type=jnp.float32).astype(jnp.bfloat16).reshape(BATCH_ROWS, KV_HEADS, HEAD_DIM)
    score_scale = HEAD_DIM ** -0.5
    positions = jnp.arange(SEQ_LEN)

    def one_sequence(row_args):
        q_row, k_row, v_row, k_self, v_self, length = row_args
        q_wide = q_row.astype(jnp.float32)
        scores = jnp.einsum('kgd,skd->kgs', q_wide, k_row.astype(jnp.float32)) * score_scale
        scores = jnp.where(positions < length, scores, -jnp.inf)
        self_score = jnp.einsum('kgd,kd->kg', q_wide, k_self.astype(jnp.float32)) * score_scale
        row_max = jnp.maximum(jnp.max(scores, axis=-1), self_score)
        weights = jnp.exp(scores - row_max[..., None])
        self_weight = jnp.exp(self_score - row_max)
        weight_sum = jnp.sum(weights, axis=-1) + self_weight
        narrow_w = weights.astype(jnp.bfloat16).astype(jnp.float32)
        weighted = jnp.einsum('kgs,skd->kgd', narrow_w, v_row.astype(jnp.float32))
        weighted = weighted + self_weight[..., None] * v_self.astype(jnp.float32)[:, None, :]
        return (weighted / weight_sum[..., None]).astype(jnp.bfloat16)

    context = lax.map(one_sequence, (queries, k_cache, v_cache, k_new, v_new, lengths))
    attn_out = jnp.dot(context.reshape(BATCH_ROWS, Q_HEADS * HEAD_DIM), w_o, preferred_element_type=jnp.float32)
    out = (hidden.astype(jnp.float32) + attn_out).astype(jnp.bfloat16)
    return (out, k_new, v_new)
```

```python
import functools

import jax
import jax.numpy as jnp
from jax import lax
from jax.experimental import pallas as pl
from jax.experimental.pallas import tpu as pltpu
from jax.sharding import PartitionSpec as P

MESH = pl.DeviceIdType.MESH
F32 = jnp.float32
BF16 = jnp.bfloat16
NEG = float('-inf')
LANES = 128
RING = 4


def rotary_tables(lengths, head_dim):
    rot_dim = head_dim // 2
    half = rot_dim // 2
    inv_freq = 10000.0 ** (-2.0 * jnp.arange(half, dtype=F32) / rot_dim)
    angle = lengths.astype(F32)[:, None] * inv_freq
    cos, sin = jnp.cos(angle), jnp.sin(angle)
    rest = jnp.zeros((lengths.shape[0], head_dim - rot_dim), F32)
    return jnp.concatenate([cos, cos, rest + 1.0], axis=1), jnp.concatenate([-sin, sin, rest], axis=1)


def qkv_kernel(hid, gain, bias, cos, sin, wq, wk, wv, q_out, ks_out, vs_out, kn_out, vn_out, wbuf, normed, raw, pair, sem):
    rows, width = hid.shape
    q_cols, kv_cols = wq.shape[1], wk.shape[1]
    step = kv_cols
    kv_heads = kv_cols // LANES
    q_heads = q_cols // LANES
    group = q_heads // kv_heads
    q_steps = q_cols // step
    steps = q_steps + 2
    copies = [pltpu.make_async_copy(wq.at[:, pl.ds(j * step, step)], wbuf.at[j], sem.at[j]) for j in range(q_steps)]
    copies.append(pltpu.make_async_copy(wk, wbuf.at[q_steps], sem.at[q_steps]))
    copies.append(pltpu.make_async_copy(wv, wbuf.at[q_steps + 1], sem.at[q_steps + 1]))
    for c in copies:
        c.start()

    tile = 16
    scale_row = 1.0 + gain[...].astype(F32)
    bias_row = bias[...].astype(F32)

    def norm(i, _):
        r = pl.ds(pl.multiple_of(i * tile, tile), tile)
        wide = hid[r, :].astype(F32)
        centred = wide - jnp.sum(wide, axis=1, keepdims=True) * (1.0 / width)
        var = jnp.sum(centred * centred, axis=1, keepdims=True) * (1.0 / width)
        normed[r, :] = (centred * lax.rsqrt(var + 1e-5) * scale_row + bias_row).astype(BF16)
        return 0

    lax.fori_loop(0, rows // tile, norm, 0)

    lane = lax.broadcasted_iota(jnp.int32, (rows, LANES), 1)
    quarter = LANES // 4

    def rotate(u):
        swapped = jnp.where(lane < quarter, pltpu.roll(u, LANES - quarter, 1), pltpu.roll(u, quarter, 1))
        return u * cos[...] + swapped * sin[...]

    for j in range(steps):
        copies[j].wait()
        raw[...] = jnp.dot(normed[...], wbuf[j], preferred_element_type=F32)
        for i in range(kv_heads):
            u = raw[:, i * LANES:(i + 1) * LANES]
            if j < q_steps:
                h = j * kv_heads + i
                q_out[pl.ds(h, rows, stride=q_heads), :] = rotate(u).astype(BF16).astype(F32)
                continue
            if j == q_steps:
                u = rotate(u)
            u = u.astype(BF16).astype(F32)
            pair[pl.ds(i, rows, stride=kv_heads), :] = u
            spread = ks_out if j == q_steps else vs_out
            for g in range(group):
                spread[pl.ds(i * group + g, rows, stride=q_heads), :] = u
        if j == q_steps:
            kn_out[...] = pair[...].astype(BF16)
        if j == q_steps + 1:
            vn_out[...] = pair[...].astype(BF16)


def main_kernel(q, kself, vself, lens, k_hbm, v_hbm, wo_hbm, hid_hbm, out, kbuf, vbuf, wo, hid, part, from_core, relay, ctx32, ctx,
                prod, in_tp, full, kv_sem, wo_sem, hid_sem, d_send, d_recv, r_send, r_recv, u_send, u_recv, a_send, a_recv,
                b_send, b_recv, g_send, g_recv):
    dp, tp, sp = lax.axis_index('dp'), lax.axis_index('tp'), lax.axis_index('sp')
    core, x, y = sp % 2, sp // 2, tp
    blocks, rows = part.shape[0], hid.shape[0]
    heads = q.shape[0] // lens.shape[0]
    keys = kbuf.shape[1] // rows
    kv_local = 2
    seq = keys // kv_local
    group = heads // kv_local
    cols = hid.shape[1]
    stat = rows * heads
    turn = 1 - 2 * core

    def at(dx, dy, c):
        return {'dp': dp, 'tp': (y + dy + RING) % RING, 'sp': ((x + dx + RING) % RING) * 2 + c}

    def remote(src, dst, send, recv, to):
        return pltpu.make_async_remote_copy(src_ref=src, dst_ref=dst, send_sem=send, recv_sem=recv, device_id=to, device_id_type=MESH)

    partner = at(0, 0, 1 - core)
    neighbours = [partner, at(1, 0, core), at(-1, 0, core), at(0, 1, core), at(0, -1, core)]
    barrier = pltpu.get_barrier_semaphore()
    for to in neighbours:
        pl.semaphore_signal(barrier, inc=1, device_id=to, device_id_type=MESH)

    def order(c):
        t = 1 - 2 * c
        return [((x + d + RING) % RING) * 2 + c for d in (2, -t, t, 0)]

    mine, theirs = order(core), order(1 - core)
    sequence = [b for pair in zip(theirs, mine) for b in pair]
    kv_copies = []
    for i, b in enumerate(sequence):
        src = pl.ds(pl.multiple_of(b * rows * keys, rows * keys), rows * keys)
        kv_copies.append((pltpu.make_async_copy(k_hbm.at[src, :], kbuf.at[i], kv_sem.at[0, i]),
                          pltpu.make_async_copy(v_hbm.at[src, :], vbuf.at[i], kv_sem.at[1, i])))
        kv_copies[i][0].start()
        kv_copies[i][1].start()
    col_order = [(y + d + RING) % RING for d in (2, -turn, turn, 0)]
    wo_copies = [pltpu.make_async_copy(wo_hbm.at[:, pl.ds(pl.multiple_of(b * cols, cols), cols)], wo.at[i], wo_sem.at[i])
                 for i, b in enumerate(col_order)]
    for c in wo_copies:
        c.start()
    hid_copy = pltpu.make_async_copy(hid_hbm.at[pl.ds(pl.multiple_of(sp * rows, rows), rows), pl.ds(pl.multiple_of(tp * cols, cols), cols)],
                                     hid, hid_sem)
    hid_copy.start()

    key_id = lax.broadcasted_iota(jnp.int32, (heads, keys), 1)
    head_id = lax.broadcasted_iota(jnp.int32, (heads, keys), 0)
    position = jnp.where(key_id % kv_local == head_id // group, key_id // kv_local, 2 ** 30)
    lane = lax.broadcasted_iota(jnp.int32, (heads, LANES), 1)
    score_scale = LANES ** -0.5
    unroll = min(8, rows)

    def attend(i):
        b = sequence[i]
        for c in kv_copies[i]:
            c.wait()

        def some(it, carry):
            m_all, l_all = carry
            for u in range(unroll):
                r = it * unroll + u
                row = b * rows + r
                qh = pl.ds(pl.multiple_of(row * heads, heads), heads)
                kh = pl.ds(pl.multiple_of(r * keys, keys), keys)
                query = q[qh, :]
                s = lax.dot_general(query.astype(BF16), kbuf[i, kh, :], (((1,), (1,)), ((), ())), preferred_element_type=F32) * score_scale
                n = lens[row] - sp * seq
                s = jnp.where(position < n, s, NEG)
                owner = jnp.where(jnp.logical_and(n >= 0, n < seq), 0.0, NEG)
                s_self = jnp.sum(query * kself[qh, :], axis=1, keepdims=True) * score_scale + owner
                m = jnp.maximum(jnp.max(s, axis=1, keepdims=True), s_self)
                safe = jnp.where(m == NEG, 0.0, m)
                w = jnp.exp(s - safe)
                w_self = jnp.exp(s_self - safe)
                total = jnp.sum(w, axis=1, keepdims=True) + w_self
                o = jnp.dot(w.astype(BF16), vbuf[i, kh, :], preferred_element_type=F32) + w_self * vself[qh, :]
                part[i, pl.ds(pl.multiple_of(r * heads, heads), heads), :] = o
                m_all = jnp.where(lane == r, m, m_all)
                l_all = jnp.where(lane == r, total, l_all)
            return m_all, l_all

        m_all, l_all = lax.fori_loop(0, rows // unroll, some, (jnp.zeros((heads, LANES), F32), jnp.ones((heads, LANES), F32)))
        part[i, stat:stat + heads, :] = m_all
        part[i, stat + heads:stat + 2 * heads, :] = l_all

    def combine(sources, last=False):
        ms = [s[stat:stat + heads, :] for s in sources]
        top = functools.reduce(jnp.maximum, ms)
        safe = jnp.where(top == NEG, 0.0, top)
        fs = [jnp.exp(m - safe) for m in ms]
        total = functools.reduce(jnp.add, [f * s[stat + heads:stat + 2 * heads, :] for f, s in zip(fs, sources)])
        if last:
            fs = [f / total for f in fs]
        for r in range(rows):
            span = slice(r * heads, (r + 1) * heads)
            acc = functools.reduce(jnp.add, [s[span, :] * f[:, r:r + 1] for f, s in zip(fs, sources)])
            if last:
                ctx32[span, :] = acc
            else:
                sources[0][span, :] = acc
        if not last:
            sources[0][stat:stat + heads, :] = top
            sources[0][stat + heads:stat + 2 * heads, :] = total

    with_turn, against = at(turn, 0, core), at(-turn, 0, core)
    cross = [remote(part.at[2 * k], from_core.at[k], d_send.at[k], d_recv.at[k], partner) for k in range(4)]
    hops = [remote(part.at[1], relay.at[0], r_send.at[0], r_recv.at[0], with_turn),
            remote(part.at[3], relay.at[2], r_send.at[2], r_recv.at[2], against),
            remote(part.at[5], relay.at[1], r_send.at[1], r_recv.at[1], with_turn)]
    for k in range(4):
        attend(2 * k)
        if k == 0:
            pl.semaphore_wait(barrier, len(neighbours))
        cross[k].start()
        attend(2 * k + 1)
        cross[k].wait_recv()
        sources = [part.at[2 * k + 1], from_core.at[k]]
        if k == 2:
            hops[0].wait_recv()
            sources.append(relay.at[0])
        if k == 3:
            hops[2].wait_recv()
            hops[1].wait_recv()
            sources += [relay.at[1], relay.at[2]]
        combine(sources, last=k == 3)
        if k < 3:
            hops[k].start()

    for h in range(heads):
        ctx[:, h * LANES:(h + 1) * LANES] = ctx32[pl.ds(h, rows, stride=heads), :].astype(BF16)

    up, down = at(0, turn, core), at(0, -turn, core)
    halves = 2
    half = rows // halves
    lands = [0, 2, 1]
    out_tp = []
    for k in range(3):
        pieces = []
        for p in range(halves):
            span = pl.ds(p * half, half)
            pieces.append(remote(prod.at[k, span, :], in_tp.at[lands[k], span, :], u_send.at[lands[k], p], u_recv.at[lands[k], p],
                                 down if k == 1 else up))
        out_tp.append(pieces)
    tile = min(cols, 512)
    for k in range(4):
        wo_copies[k].wait()
        for t in range(0, cols, tile):
            prod[k, :, t:t + tile] = jnp.dot(ctx[...], wo[k, :, t:t + tile], preferred_element_type=F32)
        if k < 2:
            for piece in out_tp[k]:
                piece.start()
    for p in range(halves):
        span = pl.ds(p * half, half)
        out_tp[0][p].wait_recv()
        prod[2, span, :] = prod[2, span, :] + in_tp[0, span, :]
        out_tp[2][p].start()
    hid_copy.wait()
    for p in range(halves):
        span = pl.ds(p * half, half)
        out_tp[1][p].wait_recv()
        out_tp[2][p].wait_recv()
        full[sp, tp, span, :] = hid[span, :].astype(F32) + (prod[3, span, :] + in_tp[2, span, :] + in_tp[1, span, :])

    offset = (0, -1, 1, 2)

    def place(c, k1, k2):
        o1, o2 = offset[k1], offset[k2]
        cx = (x + o1 * (1 - c) + o2 * c + RING) % RING
        cy = (y + o1 * c + o2 * (1 - c) + RING) % RING
        return cx * 2 + c, cy

    def chunk(c, k1, k2, piece=None):
        s, t = place(c, k1, k2)
        if piece is None:
            return full.at[s, t]
        return full.at[s, t, pl.ds(piece * half, half), :]

    def narrow(c, k1, k2):
        s, t = place(c, k1, k2)
        out[pl.ds(pl.multiple_of(s * rows, rows), rows), pl.ds(pl.multiple_of(t * cols, cols), cols)] = full[s, t].astype(BF16)

    first = [at(1 - core, core, core), at(core - 1, -core, core)]
    second = [at(core, 1 - core, core), at(-core, core - 1, core)]
    started = []

    def go(copy):
        copy.start()
        started.append(copy)

    def arrived(view, recv):
        remote(view, view, recv, recv, partner).wait_recv()

    def spread(k1):
        for d in range(2):
            go(remote(chunk(core, k1, 0), chunk(core, k1, 0), b_send.at[k1, d], b_recv.at[k1, d], second[d]))
        share(k1, 0)

    def share(k1, k2):
        go(remote(chunk(core, k1, k2), chunk(core, k1, k2), g_send.at[k1, k2], g_recv.at[k1, k2], partner))
        narrow(core, k1, k2)

    def along(k1):
        for d in range(2):
            arrived(chunk(core, k1, 1 + d), b_recv.at[k1, d])
            go(remote(chunk(core, k1, 1 + d, d), chunk(core, k1, 1 + d, d), b_send.at[k1, 2 + d], b_recv.at[k1, 2 + d], second[d]))
            share(k1, 1 + d)

    def far(k1):
        for d in range(2):
            arrived(chunk(core, k1, 3, d), b_recv.at[k1, 2 + d])
        share(k1, 3)

    for d in range(2):
        go(remote(chunk(core, 0, 0), chunk(core, 0, 0), a_send.at[d], a_recv.at[d], first[d]))
    spread(0)
    for d in range(2):
        arrived(chunk(core, 1 + d, 0), a_recv.at[d])
        go(remote(chunk(core, 1 + d, 0, d), chunk(core, 1 + d, 0, d), a_send.at[2 + d], a_recv.at[2 + d], first[d]))
        spread(1 + d)
    along(0)
    for d in range(2):
        arrived(chunk(core, 3, 0, d), a_recv.at[2 + d])
    spread(3)
    along(1)
    along(2)
    far(0)
    along(3)
    far(1)
    far(2)
    far(3)
    turns = [(0, 0), (1, 0), (2, 0), (0, 1), (0, 2), (3, 0), (1, 1), (1, 2), (2, 1), (2, 2), (0, 3), (3, 1), (3, 2), (1, 3), (2, 3), (3, 3)]
    for k1, k2 in turns:
        arrived(chunk(1 - core, k1, k2), g_recv.at[k1, k2])
        narrow(1 - core, k1, k2)
    for copy in cross + hops + [p for pieces in out_tp for p in pieces] + started:
        copy.wait_send()


def solution(mesh):
    tp_size, sp_size = mesh.shape['tp'], mesh.shape['sp']
    assert tp_size == RING and sp_size == 2 * RING

    def local_step(hidden, ln_gain, ln_bias, w_q, w_k, w_v, w_o, k_cache, v_cache, lengths):
        batch, seq_local, kv_local, head_dim = k_cache.shape
        assert head_dim == LANES and kv_local == 2
        width = hidden.shape[1]
        heads = w_q.shape[1] // head_dim
        step = w_k.shape[1]
        steps = w_q.shape[1] // step + 2
        rows, cols = batch // sp_size, w_o.shape[1] // tp_size
        keys = seq_local * kv_local
        cos, sin = rotary_tables(lengths, head_dim)
        vmem = pl.BlockSpec(memory_space=pltpu.VMEM)
        hbm = pl.BlockSpec(memory_space=pl.ANY)
        smem = pl.BlockSpec(memory_space=pltpu.SMEM)
        flat = jax.ShapeDtypeStruct((batch * heads, head_dim), F32)
        new = jax.ShapeDtypeStruct((batch * kv_local, head_dim), BF16)
        q, kself, vself, k_new, v_new = pl.pallas_call(
            qkv_kernel,
            out_shape=(flat, flat, flat, new, new),
            in_specs=[vmem] * 5 + [hbm] * 3,
            out_specs=(vmem,) * 5,
            scratch_shapes=[
                pltpu.VMEM((steps, width, step), BF16),
                pltpu.VMEM((batch, width), BF16),
                pltpu.VMEM((batch, step), F32),
                pltpu.VMEM((batch * kv_local, head_dim), F32),
                pltpu.SemaphoreType.DMA((steps,)),
            ],
            compiler_params=pltpu.CompilerParams(vmem_limit_bytes=40 * 2 ** 20),
            name='qkv',
        )(hidden, ln_gain.reshape(1, -1), ln_bias.reshape(1, -1), cos, sin, w_q, w_k, w_v)
        blocks = sp_size
        slab = rows * heads + 2 * heads
        dma = pltpu.SemaphoreType.DMA
        out = pl.pallas_call(
            main_kernel,
            out_shape=jax.ShapeDtypeStruct((batch, w_o.shape[1]), BF16),
            in_specs=[vmem] * 3 + [smem] + [hbm] * 4,
            out_specs=vmem,
            scratch_shapes=[
                pltpu.VMEM((blocks, rows * keys, head_dim), BF16),
                pltpu.VMEM((blocks, rows * keys, head_dim), BF16),
                pltpu.VMEM((tp_size, w_o.shape[0], cols), BF16),
                pltpu.VMEM((rows, cols), BF16),
                pltpu.VMEM((blocks, slab, head_dim), F32),
                pltpu.VMEM((4, slab, head_dim), F32),
                pltpu.VMEM((3, slab, head_dim), F32),
                pltpu.VMEM((rows * heads, head_dim), F32),
                pltpu.VMEM((rows, w_o.shape[0]), BF16),
                pltpu.VMEM((4, rows, cols), F32),
                pltpu.VMEM((3, rows, cols), F32),
                pltpu.VMEM((sp_size, tp_size, rows, cols), F32),
                dma((2, blocks)), dma((4,)), dma,
                dma((4,)), dma((4,)), dma((3,)), dma((3,)), dma((3, 2)), dma((3, 2)),
                dma((4,)), dma((4,)), dma((4, 4)), dma((4, 4)), dma((4, 4)), dma((4, 4)),
            ],
            compiler_params=pltpu.CompilerParams(vmem_limit_bytes=62 * 2 ** 20, collective_id=0, has_side_effects=True),
            name='attend_sum_gather',
        )(q, kself, vself, lengths, k_cache.reshape(-1, head_dim), v_cache.reshape(-1, head_dim), w_o, hidden)
        shape = (batch, kv_local, head_dim)
        return out, k_new.reshape(shape), v_new.reshape(shape)

    row_spec = P('dp', None)
    cache_spec = P('dp', 'sp', 'tp', None)
    head_spec = P('dp', 'tp', None)
    return jax.shard_map(local_step, mesh=mesh, in_specs=(row_spec, P(None), P(None), P(None, 'tp'), P(None, 'tp'), P(None, 'tp'), P('tp', None), cache_spec, cache_spec, P('dp')), out_specs=(row_spec, head_spec, head_spec), check_vma=False)
```
